32 devices in a mesh: lat: 16 (over z, y, x), fld: 2 (over core).
Axes of the slice: x: 2, y: 2, z: 4, core: 2. Of those that a mesh axis runs over, the one named last changes fastest.
Arguments:
- grid: bfloat16 [2, 4, 69, 640, 1408], P('fld', None, None, 'lat'), may hold values from -6 to 6
- cycle_ids: int32 [640], replicated, may hold values from 0 to 639, each once
- cycle_len: int32 [640], replicated, may hold values from 20 to 1296, as said below
- wave_ids: int32 [320], replicated, may hold values from 0 to 319, each once
- legendre: bfloat16 [320, 320, 640], P('lat'), may hold values from -0.25 to 0.25
- target: float32 [2, 4, 69, 2, 320, 320], P('fld', None, None, None, 'lat'), may hold values from -18 to 18
- step_w: float32 [2], P('fld'), may hold values from 0.5 to 2
- chan_w: float32 [69], replicated, may hold values from 0.2 to 2
Outputs:
- coeffs: float32 [2, 4, 69, 2, 320, 320], P('fld', None, None, None, 'lat')
- loss: float32 [], replicated
- field_grad: bfloat16 [2, 4, 69, 640, 1408], P('fld', None, None, 'lat')
The draws below stay inside these ranges and needn't reach their ends.
Inputs may be any that keep to these rules, and one draw needn't show every extreme that they name: `cycle_len`: every length 20 + 4 j with j from 0 to 319 occurs exactly twice.
All inputs are finite; a program needn't handle non-finite values.
Results may differ from the reference program's by a relative error of at most 0.0065.
Values may be sent and summed in bfloat16 or wider, within the bound.
A program may use at most 320 MiB of HBM per device.

```python
import math
import jax
import jax.numpy as jnp
from jax import lax

R = 640
MW = 320
CH = 69
BATCH = 4
STEPS = 2
SEG = 1408


def draw_cycle_len(key, part):
    order = jax.random.permutation(jax.random.fold_in(key, 11), R).astype(jnp.int32)
    return (20 + 4 * (order // 2)).astype(jnp.int32)


def draw_target(key, part):
    shape = (STEPS, BATCH, CH, 2, MW, MW)
    slot_index = jnp.arange(MW, dtype=jnp.float32) / (MW - 1)
    values = jnp.clip(jax.random.normal(jax.random.fold_in(key, 22), shape, jnp.float32), -6.0, 6.0)
    slot_scale = 0.5 + 2.5 * slot_index
    return (values * slot_scale[:, None]).astype(jnp.float32)


def steps_of(rng, extent, cuts, least, top_value):
    factor_of, own = 1.0, jax.random.fold_in(rng, 6)
    for axis_at, parts in cuts:
        draws = jnp.exp(jax.random.uniform(jax.random.fold_in(own, axis_at), (parts,), jnp.float32, least / len(cuts), top_value / len(cuts)))
        factor_of = factor_of * jnp.repeat(draws, extent[axis_at] // parts).reshape([-1 if axis == axis_at else 1 for axis in range(len(extent))])
    return factor_of


def scatter_about(rng, dims, spread, bound, shards=(), kind=jnp.bfloat16):
    gain = steps_of(rng, dims, shards, -0.22, 0.18) if shards else 1.0
    result = jax.random.normal(rng, dims, jnp.float32) * spread * gain
    return jnp.minimum(jnp.maximum(result, -bound), bound).astype(kind)


def setup_inputs(seed: int = 0) -> dict:
    keys = jax.random.split(jax.random.key(seed), 9)
    return {
        "grid": scatter_about(keys[0], (STEPS, BATCH, CH, R, SEG), 1.0, 6.0, ((0, 2), (3, 16))),
        "cycle_ids": jax.random.permutation(keys[1], R).astype(jnp.int32),
        "cycle_len": draw_cycle_len(jax.random.fold_in(keys[8], 71), 0),
        "wave_ids": jax.random.permutation(keys[3], MW).astype(jnp.int32),
        "legendre": scatter_about(keys[4], (MW, MW, R), R ** -0.5, 0.25, ((0, 16),)),
        "target": draw_target(jax.random.fold_in(keys[8], 71), 0),
        "step_w": jnp.clip(jnp.exp(math.log(2.0) - 1.3862944 * jax.random.uniform(keys[6], (STEPS,), jnp.float32) ** steps_of(keys[6], (STEPS,), ((0, 2),), -0.2, 0.2)), 0.5, 2.0),
        "chan_w": jnp.clip(jnp.exp(jax.random.uniform(keys[7], (CH,), jnp.float32, math.log(0.2), math.log(2.0))), 0.2, 2.0),
    }


def cycle_table(length, wave_order, segment):
    slot_index = jnp.arange(segment, dtype=jnp.int32)
    phase_int = slot_index[:, None] * wave_order[None, :] % length
    angles = 2.0 * math.pi / length.astype(jnp.float32) * phase_int.astype(jnp.float32)
    inside = (slot_index[:, None] < length) & (2 * wave_order[None, :] < length)
    row_scale = jnp.where(inside, lax.rsqrt(length.astype(jnp.float32)), jnp.float32(0.0))
    paired = jnp.stack([jnp.cos(angles) * row_scale, -jnp.sin(angles) * row_scale], axis=2)
    return paired.reshape(segment, 2 * wave_order.shape[0]).astype(jnp.bfloat16)

def reference(grid, cycle_ids, cycle_len, wave_ids, legendre, target, step_w, chan_w):
    step_count, batch_size, chan_count, cycle_count, segment = grid.shape
    wave_count = wave_ids.shape[0]
    col_count = step_count * batch_size * chan_count
    highest = lax.Precision.HIGHEST

    def forward_cycle(cycle_slot):
        length = cycle_len[cycle_ids[cycle_slot]]
        dft_table = cycle_table(length, wave_ids, segment).astype(jnp.float32)
        grid_rows = lax.dynamic_index_in_dim(grid, cycle_slot, 3, keepdims=False)
        grid_rows = grid_rows.reshape(col_count, segment).astype(jnp.float32)
        return jnp.dot(grid_rows, dft_table, precision=highest).astype(jnp.bfloat16)
    fourier = lax.map(forward_cycle, jnp.arange(cycle_count, dtype=jnp.int32))
    fourier = fourier.reshape(cycle_count, col_count, wave_count, 2)
    basis_all = jnp.take(legendre, cycle_ids, axis=2)
    degree = jnp.arange(wave_count, dtype=jnp.int32)
    weight_cols = jnp.broadcast_to(step_w[:, None, None] * chan_w[None, None, :], (step_count, batch_size, chan_count)).reshape(col_count)

    def per_slot(wave_slot):
        basis = lax.dynamic_index_in_dim(basis_all, wave_slot, 0, keepdims=False).astype(jnp.float32)
        slot_fourier = lax.dynamic_index_in_dim(fourier, wave_slot, 2, keepdims=False)
        slot_fourier = slot_fourier.astype(jnp.float32).reshape(cycle_count, col_count * 2)
        coeffs = jnp.dot(basis, slot_fourier, precision=highest).reshape(wave_count, col_count, 2)
        wave_num = wave_ids[wave_slot]
        kept_mask = (degree >= wave_num).astype(jnp.float32)[:, None, None]
        coeffs = coeffs * kept_mask
        target_slot = lax.dynamic_index_in_dim(target, wave_slot, 4, keepdims=False)
        target_slot = jnp.transpose(target_slot.reshape(col_count, 2, wave_count), (2, 0, 1))
        factor = jnp.where(wave_num == 0, 1.0, 2.0).astype(jnp.float32)
        weight = (factor * weight_cols)[None, :, None]
        misfit = (coeffs - target_slot) * kept_mask
        partial_value = jnp.sum(weight * misfit * misfit)
        grad_coeff = (2.0 * weight * misfit).astype(jnp.bfloat16)
        back_rows = jnp.dot(basis.T, grad_coeff.astype(jnp.float32).reshape(wave_count, col_count * 2), precision=highest).astype(jnp.bfloat16)
        return (jnp.transpose(coeffs, (1, 2, 0)), partial_value, back_rows.reshape(cycle_count, col_count, 2))
    coeff_all, partials, back_all = lax.map(per_slot, jnp.arange(wave_count, dtype=jnp.int32))
    coeff_all = coeff_all.reshape(wave_count, step_count, batch_size, chan_count, 2, wave_count)
    coeffs = jnp.moveaxis(coeff_all, 0, 4)

    def adjoint_cycle(cycle_slot):
        length = cycle_len[cycle_ids[cycle_slot]]
        dft_table = cycle_table(length, wave_ids, segment).astype(jnp.float32)
        slot_back = lax.dynamic_index_in_dim(back_all, cycle_slot, 1, keepdims=False)
        slot_back = jnp.transpose(slot_back, (1, 0, 2)).reshape(col_count, 2 * wave_count)
        return jnp.dot(slot_back.astype(jnp.float32), dft_table.T, precision=highest).astype(jnp.bfloat16)
    field_rows = lax.map(adjoint_cycle, jnp.arange(cycle_count, dtype=jnp.int32))
    field_rows = field_rows.reshape(cycle_count, step_count, batch_size, chan_count, segment)
    field_grad = jnp.moveaxis(field_rows, 0, 3)
    term_count = step_count * batch_size * chan_count * wave_count * (wave_count + 1) // 2
    loss = jnp.sum(partials) / jnp.float32(term_count)
    return (coeffs, loss, field_grad)
```

```python
import functools
import math

import jax
import jax.numpy as jnp
from jax import lax
from jax.experimental import pallas as pl
from jax.experimental.pallas import tpu as pltpu
from jax.sharding import PartitionSpec as P


STEPS = 2
LANES = 128
SUB = 8
RUN = 64
WAVES_STEP = 5
PIECE = 24


def sin_cos(length, product, inverse=None):
    if inverse is None:
        inverse = 1.0 / length.astype(jnp.float32)
    quarter = jnp.floor(product.astype(jnp.float32) * (4.0 * inverse) + 0.5).astype(jnp.int32)
    rest = 4 * product - quarter * length
    x = rest.astype(jnp.float32) * ((0.5 * math.pi) * inverse)
    x2 = x * x
    sin_x = x + x * x2 * (
        -1.0 / 6 + x2 * (1.0 / 120 + x2 * (-1.0 / 5040 + x2 * (1.0 / 362880)))
    )
    cos_x = 1.0 + x2 * (
        -0.5 + x2 * (1.0 / 24 + x2 * (-1.0 / 720 + x2 * (1.0 / 40320 - x2 * (1.0 / 3628800))))
    )
    odd = (quarter & 1) == 1
    sine = jnp.where(odd, cos_x, sin_x)
    cosine = jnp.where(odd, sin_x, cos_x)
    sine = jnp.where((quarter & 2) == 2, -sine, sine)
    cosine = jnp.where(((quarter + 1) & 2) == 2, -cosine, cosine)
    return sine, cosine


def make_table(length, inverse, root, wave_ref, sine_ref, table_ref):
    segment, width = table_ref.shape

    def lane_tile(tile, carry):
        lanes = pl.ds(pl.multiple_of(tile * LANES, LANES), LANES)
        wave = wave_ref[:, lanes]
        is_sine = sine_ref[:, lanes] == 1
        row = lax.broadcasted_iota(jnp.int32, (RUN, LANES), 0)
        scale = jnp.where(2 * wave < length, root, 0.0)
        sin_k, cos_k = sin_cos(length, row * wave, inverse)
        sin_run, cos_run = sin_cos(length, RUN * wave, inverse)
        before = jnp.where(is_sine, -sin_k, cos_k) * scale
        slope = jnp.where(is_sine, -cos_k, -sin_k) * scale
        now = before * cos_run + slope * sin_run
        twice = 2.0 * cos_run
        for step in range(segment // RUN):
            value = jnp.where(row < length - step * RUN, before, 0.0)
            table_ref[pl.ds(step * RUN, RUN), lanes] = value.astype(jnp.bfloat16)
            before, now = now, twice * now - before
        return carry

    lax.fori_loop(0, width // LANES, lane_tile, 0)


def forward_kernel(
    lat, first, groups, len_ref, inv_ref, root_ref, wave_ref, sine_ref, grid_ref, *rest
):
    outs, (rows_ref, table_ref, flat_ref, main_ref, tail_ref) = rest[:-5], rest[-5:]
    cols, _, segment = grid_ref.shape
    width = table_ref.shape[1]
    whole = cols // LANES * LANES
    per_tile = 2 * WAVES_STEP // 2
    block = pl.program_id(0) + first
    chunk = 12 if cols % 12 == 0 else 1

    def widen(i, carry):
        part = grid_ref[pl.ds(i * chunk, chunk), :, :].astype(jnp.float32)
        start = pl.multiple_of(i * chunk * SUB, SUB)
        for t in range(segment // LANES):
            piece = part[:, :, t * LANES : (t + 1) * LANES]
            rows_ref[t, pl.ds(start, chunk * SUB), :] = piece.reshape(chunk * SUB, LANES)
        return carry

    lax.fori_loop(0, cols // chunk, widen, 0)
    pad = flat_ref.shape[0]
    flat_ref[cols // SUB * SUB :, :] = jnp.zeros((pad - cols // SUB * SUB, width), jnp.float32)

    def cycle(r, carry):
        slot = block * SUB + r
        make_table(len_ref[slot], inv_ref[slot], root_ref[slot], wave_ref, sine_ref, table_ref)
        rows = [
            rows_ref[t, pl.ds(r, cols, stride=SUB), :].astype(jnp.bfloat16)
            for t in range(segment // LANES)
        ]
        rows = jnp.concatenate(rows, axis=1)
        flat_ref[:cols, :] = jnp.dot(rows, table_ref[...], preferred_element_type=jnp.float32)
        for h in range(whole // LANES):
            value = flat_ref[h * LANES : (h + 1) * LANES, :].T
            main_ref[h, pl.ds(r, width, stride=SUB), :] = value
        tail = flat_ref[whole:, :].T.reshape(width // lat, lat, LANES)
        for t in range(width // lat // per_tile):
            total = tail[t * per_tile]
            for i in range(1, per_tile):
                total = total + pltpu.roll(tail[t * per_tile + i], PIECE * i, axis=1)
            tail_ref[pl.ds(t * lat * SUB + r, lat, stride=SUB), :] = total
        return carry

    lax.fori_loop(0, SUB, cycle, 0)

    halves = whole // LANES
    mains = 2 * WAVES_STEP * halves

    def deliver(owner, carry):
        quarter = 0
        for out_ref, quarters in zip(outs, groups):
            for q in range(quarters):
                for jj in range(2 * WAVES_STEP):
                    start = ((quarter * 2 * WAVES_STEP + jj) * lat + owner) * SUB
                    for h in range(halves):
                        piece = main_ref[h, pl.ds(pl.multiple_of(start, SUB), SUB), :]
                        out_ref[owner, 0, q, jj * halves + h] = piece.astype(jnp.bfloat16)
                for t in range(2):
                    start = ((quarter * 2 + t) * lat + owner) * SUB
                    value = tail_ref[pl.ds(pl.multiple_of(start, SUB), SUB), :]
                    out_ref[owner, 0, q, mains + t] = value.astype(jnp.bfloat16)
                quarter += 1
        return carry

    lax.fori_loop(0, lat, deliver, 0)


def forward(lat, first, blocks, groups, lengths, inverse, root, waves, sine, rows):
    cols, _, segment = rows.shape
    width = waves.shape[1]
    whole = cols // LANES * LANES
    tiles = 2 * WAVES_STEP * (whole // LANES) + 2
    smem = pl.BlockSpec(memory_space=pltpu.SMEM)
    small = pl.BlockSpec((1, width), lambda b: (0, 0))
    return pl.pallas_call(
        functools.partial(forward_kernel, lat, first, groups),
        grid=(blocks,),
        in_specs=[smem, smem, smem, small, small]
        + [pl.BlockSpec((cols, SUB, segment), lambda b: (0, b + first, 0))],
        out_specs=[
            pl.BlockSpec((lat, 1, q, tiles, SUB, LANES), lambda b: (0, b, 0, 0, 0, 0)) for q in groups
        ],
        out_shape=[
            jax.ShapeDtypeStruct((lat, blocks, q, tiles, SUB, LANES), jnp.bfloat16) for q in groups
        ],
        scratch_shapes=[
            pltpu.VMEM((segment // LANES, cols * SUB, LANES), jnp.float32),
            pltpu.VMEM((segment, width), jnp.bfloat16),
            pltpu.VMEM((whole + LANES, width), jnp.float32),
            pltpu.VMEM((whole // LANES, width * SUB, LANES), jnp.float32),
            pltpu.VMEM((width // WAVES_STEP * SUB, LANES), jnp.float32),
        ],
        compiler_params=pltpu.CompilerParams(vmem_limit_bytes=58 * 2**20),
        cost_estimate=pl.CostEstimate(
            flops=2 * cols * segment * width * SUB * blocks,
            bytes_accessed=2 * cols * (segment + width) * SUB * blocks,
            transcendentals=0,
        ),
        name="forward_cycles",
    )(lengths, inverse, root, waves, sine, rows)


def middle_kernel(lat, parts, wave_ref, weight_ref, legendre_ref, target_ref, *rest):
    ins = rest[: len(parts[0])]
    rest = rest[len(parts[0]) :]
    coeff_ref, loss_ref = rest[:2]
    outs, (grad_tail, flat_ref) = rest[2:-2], rest[-2:]
    cols, degrees = weight_ref.shape
    cycles = legendre_ref.shape[2]
    whole = cols // LANES * LANES
    halves = whole // LANES
    mains = 2 * WAVES_STEP * halves
    per_tile = WAVES_STEP
    rows = lat * SUB
    step = pl.program_id(0)
    degree = lax.broadcasted_iota(jnp.int32, (cols, degrees), 1)

    @pl.when(step == 0)
    def _():
        loss_ref[...] = jnp.zeros_like(loss_ref)

    grad_tail[...] = jnp.zeros_like(grad_tail)
    flat_ref[cols // SUB * SUB :, :] = jnp.zeros(
        (flat_ref.shape[0] - cols // SUB * SUB, cycles), jnp.float32
    )

    def one(jj, carry):
        s, part = jj // 2, jj % 2
        tile, place = jj // per_tile, jj % per_tile
        pieces = []
        for ref, count in zip(ins, parts[0]):
            for b in range(count):
                lanes = [
                    ref[:, b, 0, jj * halves + h].reshape(rows, LANES) for h in range(halves)
                ]
                tail = ref[:, b, 0, mains + tile].reshape(rows, LANES).astype(jnp.float32)
                shift = lax.rem(LANES - PIECE * place, LANES)
                lanes.append(pltpu.roll(tail, shift, axis=1).astype(jnp.bfloat16))
                pieces.append(jnp.concatenate(lanes, axis=1))
        fourier = jnp.concatenate(pieces, axis=0)[:, :cols]
        basis = legendre_ref[s]
        coeffs = lax.dot_general(
            fourier, basis, (((0,), (1,)), ((), ())), preferred_element_type=jnp.float32
        )
        keep = degree >= wave_ref[step * WAVES_STEP + s]
        coeffs = jnp.where(keep, coeffs, 0.0)
        coeff_ref[s, part] = coeffs
        misfit = jnp.where(keep, coeffs - target_ref[s, part], 0.0)
        factor = jnp.where(wave_ref[step * WAVES_STEP + s] == 0, 1.0, 2.0)
        slope = (factor * weight_ref[...]) * misfit
        loss_ref[...] += jnp.sum(slope * misfit, axis=0, keepdims=True)
        grad = (2.0 * slope).astype(jnp.bfloat16)
        flat_ref[:cols, :] = jnp.dot(grad, basis, preferred_element_type=jnp.float32)
        main = flat_ref[:whole, :].T
        tail = flat_ref[whole:, :].T
        offset = 0
        for ref, count in zip(outs, parts[1]):
            for b in range(count):
                for h in range(halves):
                    value = main[offset : offset + rows, h * LANES : (h + 1) * LANES]
                    ref[:, b, 0, jj * halves + h] = value.astype(jnp.bfloat16).reshape(
                        lat, SUB, LANES
                    )
                offset += rows
        grad_tail[tile] += pltpu.roll(tail, PIECE * place, axis=1)
        return carry

    lax.fori_loop(0, 2 * WAVES_STEP, one, 0)
    for tile in range(2):
        offset = 0
        for ref, count in zip(outs, parts[1]):
            for b in range(count):
                value = grad_tail[tile, pl.ds(offset, rows), :]
                ref[:, b, 0, mains + tile] = value.astype(jnp.bfloat16).reshape(lat, SUB, LANES)
                offset += rows


def middle(lat, first, quarters, splits, waves, weight, legendre, target, arrays):
    cols, degrees = weight.shape
    cycles = legendre.shape[2]
    tiles = arrays[0][0].shape[3]
    whole = cols // LANES * LANES
    parts = (tuple(a.shape[1] for a, _ in arrays), tuple(splits))

    def tile_spec(count, start):
        return pl.BlockSpec(
            (lat, count, 1, tiles, SUB, LANES), lambda q: (0, 0, q + start, 0, 0, 0)
        )

    out_specs = [
        pl.BlockSpec((WAVES_STEP, 2, cols, degrees), lambda q: (q, 0, 0, 0)),
        pl.BlockSpec((1, degrees), lambda q: (0, 0)),
    ] + [tile_spec(count, 0) for count in splits]
    out_shape = [
        jax.ShapeDtypeStruct((quarters * WAVES_STEP, 2, cols, degrees), jnp.float32),
        jax.ShapeDtypeStruct((1, degrees), jnp.float32),
    ] + [
        jax.ShapeDtypeStruct((lat, count, quarters, tiles, SUB, LANES), jnp.bfloat16)
        for count in splits
    ]
    return pl.pallas_call(
        functools.partial(middle_kernel, lat, parts),
        grid=(quarters,),
        in_specs=[
            pl.BlockSpec(memory_space=pltpu.SMEM),
            pl.BlockSpec((cols, degrees), lambda q: (0, 0)),
            pl.BlockSpec((WAVES_STEP, degrees, cycles), lambda q: (q + first, 0, 0)),
            pl.BlockSpec((WAVES_STEP, 2, cols, degrees), lambda q: (q + first, 0, 0, 0)),
        ]
        + [tile_spec(a.shape[1], start) for a, start in arrays],
        out_specs=out_specs,
        out_shape=out_shape,
        scratch_shapes=[
            pltpu.VMEM((2, cycles, LANES), jnp.float32),
            pltpu.VMEM((whole + LANES, cycles), jnp.float32),
        ],
        compiler_params=pltpu.CompilerParams(vmem_limit_bytes=60 * 2**20),
        cost_estimate=pl.CostEstimate(
            flops=8 * cols * degrees * cycles * WAVES_STEP * quarters,
            bytes_accessed=20 * cols * degrees * WAVES_STEP * quarters,
            transcendentals=0,
        ),
        name="middle_waves",
    )(waves, weight, legendre, target, *[a for a, _ in arrays])


def backward_kernel(
    lat, first, groups, len_ref, inv_ref, root_ref, wave_ref, sine_ref, *rest
):
    ins = rest[: len(groups)]
    out_ref, rows_ref, table_ref, main_ref, tail_ref = rest[-5:]
    cols, _, segment = out_ref.shape
    width = table_ref.shape[1]
    whole = cols // LANES * LANES
    halves = whole // LANES
    mains = 2 * WAVES_STEP * halves
    per_tile = WAVES_STEP
    block = pl.program_id(0) + first

    def collect(owner, carry):
        quarter = 0
        for in_ref, quarters in zip(ins, groups):
            for q in range(quarters):
                for jj in range(2 * WAVES_STEP):
                    start = ((quarter * 2 * WAVES_STEP + jj) * lat + owner) * SUB
                    at = pl.ds(pl.multiple_of(start, SUB), SUB)
                    for h in range(halves):
                        value = in_ref[owner, 0, q, jj * halves + h].astype(jnp.float32)
                        main_ref[h, at, :] = value
                for t in range(2):
                    start = ((quarter * 2 + t) * lat + owner) * SUB
                    at = pl.ds(pl.multiple_of(start, SUB), SUB)
                    tail_ref[at, :] = in_ref[owner, 0, q, mains + t].astype(jnp.float32)
                quarter += 1
        return carry

    lax.fori_loop(0, lat, collect, 0)

    def cycle(r, carry):
        slot = block * SUB + r
        make_table(len_ref[slot], inv_ref[slot], root_ref[slot], wave_ref, sine_ref, table_ref)
        main = [main_ref[h, pl.ds(r, width, stride=SUB), :].T for h in range(halves)]
        pieces = []
        for t in range(width // lat // per_tile):
            value = tail_ref[pl.ds(t * lat * SUB + r, lat, stride=SUB), :]
            for i in range(per_tile):
                pieces.append(value if i == 0 else pltpu.roll(value, LANES - PIECE * i, axis=1))
        tail = jnp.concatenate(pieces, axis=0).T
        spectrum = jnp.concatenate([*main, tail[: cols - whole]], axis=0).astype(jnp.bfloat16)
        field = lax.dot_general(
            spectrum, table_ref[...], (((1,), (1,)), ((), ())), preferred_element_type=jnp.float32
        )
        for t in range(segment // LANES):
            piece = field[:, t * LANES : (t + 1) * LANES]
            rows_ref[t, pl.ds(r, cols, stride=SUB), :] = piece
        return carry

    lax.fori_loop(0, SUB, cycle, 0)
    chunk = 12 if cols % 12 == 0 else 1

    def narrow(i, carry):
        start = pl.multiple_of(i * chunk * SUB, SUB)
        for t in range(segment // LANES):
            value = rows_ref[t, pl.ds(start, chunk * SUB), :].reshape(chunk, SUB, LANES)
            lanes = slice(t * LANES, (t + 1) * LANES)
            out_ref[pl.ds(i * chunk, chunk), :, lanes] = value.astype(jnp.bfloat16)
        return carry

    lax.fori_loop(0, cols // chunk, narrow, 0)


def backward(lat, first, blocks, lengths, inverse, root, waves, sine, arrays, shape, done):
    cols, _, segment = shape
    width = waves.shape[1]
    whole = cols // LANES * LANES
    tiles = arrays[0][0].shape[3]
    groups = tuple(a.shape[2] for a, _ in arrays)
    smem = pl.BlockSpec(memory_space=pltpu.SMEM)
    small = pl.BlockSpec((1, width), lambda b: (0, 0))

    def tile_spec(q, start):
        return pl.BlockSpec((lat, 1, q, tiles, SUB, LANES), lambda b: (0, b + start, 0, 0, 0, 0))

    extra = [] if done is None else [done]
    in_specs = [smem, smem, smem, small, small]
    in_specs += [tile_spec(a.shape[2], start) for a, start in arrays]
    in_specs += [pl.BlockSpec(memory_space=pl.ANY)] * len(extra)
    return pl.pallas_call(
        functools.partial(backward_kernel, lat, first, groups),
        grid=(blocks,),
        in_specs=in_specs,
        out_specs=pl.BlockSpec((cols, SUB, segment), lambda b: (0, b + first, 0)),
        out_shape=jax.ShapeDtypeStruct(shape, jnp.bfloat16),
        scratch_shapes=[
            pltpu.VMEM((segment // LANES, cols * SUB, LANES), jnp.float32),
            pltpu.VMEM((segment, width), jnp.bfloat16),
            pltpu.VMEM((whole // LANES, width * SUB, LANES), jnp.float32),
            pltpu.VMEM((width // WAVES_STEP * SUB, LANES), jnp.float32),
        ],
        input_output_aliases={} if done is None else {5 + len(arrays): 0},
        compiler_params=pltpu.CompilerParams(vmem_limit_bytes=58 * 2**20),
        cost_estimate=pl.CostEstimate(
            flops=2 * cols * segment * width * SUB * blocks,
            bytes_accessed=2 * cols * (segment + width) * SUB * blocks,
            transcendentals=0,
        ),
        name="backward_cycles",
    )(lengths, inverse, root, waves, sine, *[a for a, _ in arrays], *extra)


def exchange(x):
    return lax.all_to_all(x, "lat", split_axis=0, concat_axis=0, tiled=True)


def per_device(lat, grid, cycle_ids, cycle_len, wave_ids, legendre, target, step_w, chan_w):
    _, batch_size, chan_count, cycle_dev, segment = grid.shape
    wave_count = wave_ids.shape[0]
    wave_dev, degrees, cycle_count = legendre.shape
    cols = batch_size * chan_count
    lat_index = lax.axis_index("lat")
    blocks = cycle_dev // SUB
    quarters = wave_dev // WAVES_STEP
    early = quarters // 2
    late = quarters - early
    rows = grid[0].reshape(cols, cycle_dev, segment)

    my_cycles = lax.dynamic_slice_in_dim(cycle_ids, lat_index * cycle_dev, cycle_dev)
    lengths = jnp.take(cycle_len, my_cycles)
    inverse = 1.0 / lengths.astype(jnp.float32)
    root = lax.rsqrt(lengths.astype(jnp.float32))
    by_slot = jnp.transpose(wave_ids.reshape(lat, wave_dev))
    waves = jnp.broadcast_to(by_slot[:, None, :], (wave_dev, 2, lat)).reshape(1, -1)
    sine = (jnp.arange(2 * wave_dev * lat, dtype=jnp.int32) // lat % 2).reshape(1, -1)
    tables = (lengths, inverse, root, waves, sine)

    sizes = (1, (blocks - 1) // 2, blocks - 1 - (blocks - 1) // 2)
    (out0,) = forward(lat, 0, sizes[0], (quarters,), *tables, rows)
    in0 = exchange(out0)
    (out1,) = forward(lat, sizes[0], sizes[1], (quarters,), *tables, rows)
    in1 = exchange(out1)
    out2, out3 = forward(lat, sizes[0] + sizes[1], sizes[2], (early, late), *tables, rows)
    in2 = exchange(out2)
    in3 = exchange(out3)

    order = jnp.transpose(cycle_ids.reshape(lat, blocks, SUB), (1, 0, 2)).reshape(-1)
    pick = (jnp.arange(cycle_count, dtype=jnp.int32)[:, None] == order[None, :]).astype(jnp.bfloat16)
    basis = jnp.dot(
        legendre.reshape(wave_dev * degrees, cycle_count),
        pick,
        preferred_element_type=jnp.float32,
    )
    basis = basis.astype(jnp.bfloat16).reshape(wave_dev, degrees, cycle_count)
    my_waves = lax.dynamic_slice_in_dim(wave_ids, lat_index * wave_dev, wave_dev)
    weight = jnp.broadcast_to(step_w[0] * chan_w[None, :], (batch_size, chan_count))
    weight = jnp.broadcast_to(weight.reshape(cols, 1), (cols, degrees))
    goal = jnp.transpose(target[0].reshape(cols, 2, wave_dev, degrees), (2, 1, 0, 3))

    cut = early * WAVES_STEP
    coeffs_a, loss_a, back0 = middle(
        lat, 0, early, (blocks,), my_waves[:cut], weight, basis, goal,
        [(in0, 0), (in1, 0), (in2, 0)],
    )
    ret0 = exchange(back0)
    leave = (sizes[1], sizes[2], sizes[0])
    coeffs_b, loss_b, back1, back2, back3 = middle(
        lat, early, late, leave, my_waves[cut:], weight, basis, goal,
        [(in0, early), (in1, early), (in3, 0)],
    )
    ret1 = exchange(back1)
    ret2 = exchange(back2)
    ret3 = exchange(back3)

    shape = (cols, cycle_dev, segment)
    field, start = None, 0
    for arrived, count in zip((ret1, ret2, ret3), leave):
        field = backward(lat, start, count, *tables, [(ret0, start), (arrived, 0)], shape, field)
        start += count
    field_grad = field.reshape(1, batch_size, chan_count, cycle_dev, segment)
    coeffs = jnp.concatenate([coeffs_a, coeffs_b], axis=0)
    coeff_out = jnp.transpose(coeffs, (2, 1, 0, 3)).reshape(
        1, batch_size, chan_count, 2, wave_dev, degrees
    )
    loss_sum = lax.psum(jnp.sum(loss_a + loss_b), ("lat", "fld"))
    term_count = STEPS * cols * wave_count * (wave_count + 1) // 2
    loss = loss_sum / jnp.float32(term_count)
    return (coeff_out, loss, field_grad)


def cycle_tables(lengths, waves, is_sine, segment):
    inner = math.gcd(segment, 32)
    outer = segment // inner
    length = lengths[:, None, None]
    wave = waves[None, None, :]
    coarse = (inner * jnp.arange(outer, dtype=jnp.int32))[None, :, None]
    fine = jnp.arange(inner, dtype=jnp.int32)[None, :, None]
    sin_a, cos_a = sin_cos(length, wave * coarse)
    sin_b, cos_b = sin_cos(length, wave * fine)
    scale = jnp.where(2 * wave < length, lax.rsqrt(length.astype(jnp.float32)), 0.0)
    sine = is_sine[None, None, :]
    first = jnp.where(sine, -sin_a, cos_a) * scale
    second = jnp.where(sine, -cos_a, -sin_a) * scale
    first, second, sin_b, cos_b = lax.optimization_barrier((first, second, sin_b, cos_b))
    table = first[:, :, None, :] * cos_b[:, None, :, :] + second[:, :, None, :] * sin_b[:, None, :, :]
    inside = (coarse[..., None] + fine[:, None]) < length[..., None]
    table = jnp.where(inside, table, 0.0).astype(jnp.bfloat16)
    return table.reshape(lengths.shape[0], segment, waves.shape[0])


def per_device_simple(lat, grid, cycle_ids, cycle_len, wave_ids, legendre, target, step_w, chan_w):
    _, batch_size, chan_count, cycle_dev, segment = grid.shape
    wave_count = wave_ids.shape[0]
    wave_dev, degrees, cycle_count = legendre.shape
    col_count = batch_size * chan_count
    lat_index = lax.axis_index("lat")
    my_cycles = lax.dynamic_slice_in_dim(cycle_ids, lat_index * cycle_dev, cycle_dev)
    lengths = jnp.take(cycle_len, my_cycles)

    pair = 2 * wave_dev
    by_owner = wave_ids.reshape(lat, 1, wave_dev)
    column_waves = jnp.broadcast_to(by_owner, (lat, 2, wave_dev)).reshape(-1)
    is_sine = (jnp.arange(lat * pair, dtype=jnp.int32) // wave_dev) % 2 == 1
    tables = cycle_tables(lengths, column_waves, is_sine, segment)
    tables = lax.optimization_barrier(tables)

    rows = grid[0].reshape(col_count, cycle_dev, segment)
    fourier = jnp.einsum("rkj,brk->rjb", tables, rows, preferred_element_type=jnp.float32)
    fourier = fourier.astype(jnp.bfloat16).reshape(cycle_dev, lat, pair, col_count)
    fourier = jnp.transpose(fourier, (1, 0, 2, 3))
    gathered = lax.all_to_all(fourier, "lat", split_axis=0, concat_axis=0, tiled=True)
    gathered = gathered.reshape(cycle_count, 2, wave_dev, col_count)

    legendre_cols = jnp.take(legendre, cycle_ids, axis=2)
    my_waves = lax.dynamic_slice_in_dim(wave_ids, lat_index * wave_dev, wave_dev)
    kept = jnp.arange(degrees, dtype=jnp.int32)[None, :] >= my_waves[:, None]
    kept = kept.astype(jnp.float32)[:, None, None, :]
    factor = jnp.where(my_waves == 0, 1.0, 2.0).astype(jnp.float32)
    weight_cols = jnp.broadcast_to(step_w[0] * chan_w[None, :], (batch_size, chan_count))
    weight = factor[:, None, None, None] * weight_cols.reshape(1, 1, col_count, 1)
    target_local = jnp.transpose(
        target[0].reshape(col_count, 2, wave_dev, degrees), (2, 1, 0, 3)
    )
    coeffs = jnp.einsum(
        "rpsb,snr->spbn", gathered, legendre_cols, preferred_element_type=jnp.float32
    )
    coeffs = coeffs * kept
    misfit = (coeffs - target_local) * kept
    partial_value = jnp.sum(weight * misfit * misfit)
    grad_coeff = (2.0 * weight * misfit).astype(jnp.bfloat16)
    back = jnp.einsum(
        "snr,spbn->sprb", legendre_cols, grad_coeff, preferred_element_type=jnp.float32
    )
    back = jnp.transpose(back.astype(jnp.bfloat16), (2, 1, 0, 3))
    back = back.reshape(lat, cycle_dev, pair, col_count)
    returned = lax.all_to_all(back, "lat", split_axis=0, concat_axis=0, tiled=True)
    returned = jnp.transpose(returned, (1, 0, 2, 3)).reshape(cycle_dev, lat * pair, col_count)
    field = jnp.einsum("rjb,rkj->brk", returned, tables, preferred_element_type=jnp.float32)
    field_grad = field.astype(jnp.bfloat16).reshape(
        1, batch_size, chan_count, cycle_dev, segment
    )
    coeff_out = jnp.transpose(coeffs, (2, 1, 0, 3)).reshape(
        1, batch_size, chan_count, 2, wave_dev, degrees
    )
    loss_sum = lax.psum(partial_value, ("lat", "fld"))
    term_count = STEPS * col_count * wave_count * (wave_count + 1) // 2
    loss = loss_sum / jnp.float32(term_count)
    return (coeff_out, loss, field_grad)


def tiled(lat, grid, legendre):
    _, batch_size, chan_count, cycle_dev, segment = grid.shape
    wave_dev, cols = legendre.shape[0], batch_size * chan_count
    spare = cols % LANES
    return (
        cycle_dev % SUB == 0
        and cycle_dev // SUB >= 3
        and wave_dev % (2 * WAVES_STEP) == 0
        and 2 * wave_dev * lat % LANES == 0
        and legendre.shape[2] % LANES == 0
        and lat % SUB == 0
        and segment % RUN == 0
        and segment % LANES == 0
        and cols > LANES
        and 0 < spare <= PIECE
    )


def route(lat, grid, cycle_ids, cycle_len, wave_ids, legendre, *rest):
    run = per_device if tiled(lat, grid, legendre) else per_device_simple
    return run(lat, grid, cycle_ids, cycle_len, wave_ids, legendre, *rest)


def solution(mesh):
    lat = mesh.shape["lat"]
    return jax.shard_map(
        lambda *args: route(lat, *args),
        mesh=mesh,
        in_specs=(
            P("fld", None, None, "lat", None),
            P(),
            P(),
            P(),
            P("lat", None, None),
            P("fld", None, None, None, "lat", None),
            P("fld"),
            P(),
        ),
        out_specs=(P("fld", None, None, None, "lat", None), P(), P("fld", None, None, "lat", None)),
        check_vma=False,
    )
```

```python
import functools
import math

import jax
import jax.numpy as jnp
from jax import lax
from jax.experimental import pallas as pl
from jax.experimental.pallas import tpu as pltpu
from jax.sharding import PartitionSpec as P


STEPS = 2
LANES = 128
SUB = 8
RUN = 32
WAVES_STEP = 5
TERMS = 3
SPARE = 120
PIECE = 24


def sin_cos(length, product, inverse=None):
    if inverse is None:
        inverse = 1.0 / length.astype(jnp.float32)
    quarter = jnp.floor(product.astype(jnp.float32) * (4.0 * inverse) + 0.5).astype(jnp.int32)
    rest = 4 * product - quarter * length
    x = rest.astype(jnp.float32) * ((0.5 * math.pi) * inverse)
    x2 = x * x
    sin_x = x + x * x2 * (
        -1.0 / 6 + x2 * (1.0 / 120 + x2 * (-1.0 / 5040 + x2 * (1.0 / 362880)))
    )
    cos_x = 1.0 + x2 * (
        -0.5 + x2 * (1.0 / 24 + x2 * (-1.0 / 720 + x2 * (1.0 / 40320 - x2 * (1.0 / 3628800))))
    )
    odd = (quarter & 1) == 1
    sine = jnp.where(odd, cos_x, sin_x)
    cosine = jnp.where(odd, sin_x, cos_x)
    sine = jnp.where((quarter & 2) == 2, -sine, sine)
    cosine = jnp.where(((quarter + 1) & 2) == 2, -cosine, cosine)
    return sine, cosine


def make_table(length, inverse, root, wave_ref, sine_ref, table_ref):
    segment, width = table_ref.shape

    for tile in range(width // LANES):
        lanes = slice(tile * LANES, (tile + 1) * LANES)
        wave = wave_ref[:, lanes]
        is_sine = sine_ref[:, lanes] == 1
        row = lax.broadcasted_iota(jnp.int32, (RUN, LANES), 0)
        scale = jnp.where(2 * wave < length, root, 0.0)
        sin_k, cos_k = sin_cos(length, row * wave, inverse)
        sin_run, cos_run = sin_cos(length, RUN * wave, inverse)
        before = jnp.where(is_sine, -sin_k, cos_k) * scale
        slope = jnp.where(is_sine, -cos_k, -sin_k) * scale
        now = before * cos_run + slope * sin_run
        twice = 2.0 * cos_run
        for step in range(segment // RUN):
            table_ref[pl.ds(step * RUN, RUN), lanes] = before.astype(jnp.bfloat16)
            before, now = now, twice * now - before


def forward_kernel(
    lat, first, groups, len_ref, inv_ref, root_ref, wave_ref, sine_ref, grid_ref, *rest
):
    outs, (rows_ref, even_ref, odd_ref, flat_ref, main_ref, tail_ref) = rest[:-6], rest[-6:]
    cols, _, segment = grid_ref.shape
    width = even_ref.shape[1]
    whole = cols // LANES * LANES
    per_tile = 2 * WAVES_STEP // 2
    block = pl.program_id(0) + first
    chunk = 12 if cols % 12 == 0 else 1

    def widen(i, carry):
        part = grid_ref[pl.ds(i * chunk, chunk), :, :].astype(jnp.float32)
        start = pl.multiple_of(i * chunk * SUB, SUB)
        for t in range(segment // LANES):
            piece = part[:, :, t * LANES : (t + 1) * LANES]
            rows_ref[t, pl.ds(start, chunk * SUB), :] = piece.reshape(chunk * SUB, LANES)
        return carry

    lax.fori_loop(0, cols // chunk, widen, 0)
    pad = flat_ref.shape[0]
    flat_ref[cols // SUB * SUB :, :] = jnp.zeros((pad - cols // SUB * SUB, width), jnp.float32)

    last = (first + pl.num_programs(0)) * SUB - 1

    def prepare(r, table_ref):
        slot = jnp.minimum(block * SUB + r, last)
        make_table(len_ref[slot], inv_ref[slot], root_ref[slot], wave_ref, sine_ref, table_ref)

    def cycle(r, table_ref):
        length = len_ref[block * SUB + r]
        lane = lax.broadcasted_iota(jnp.int32, (cols, LANES), 1)
        rows = []
        for t in range(segment // LANES):
            piece = rows_ref[t, pl.ds(r, cols, stride=SUB), :]
            rows.append(jnp.where(lane < length - t * LANES, piece, 0.0).astype(jnp.bfloat16))
        rows = jnp.concatenate(rows, axis=1)
        flat_ref[:cols, :] = jnp.dot(rows, table_ref[...], preferred_element_type=jnp.float32)
        for h in range(whole // LANES):
            value = flat_ref[h * LANES : (h + 1) * LANES, :].T
            main_ref[h, pl.ds(r, width, stride=SUB), :] = value
        tail = flat_ref[whole:, :].T.reshape(width // lat, lat, LANES)
        for t in range(width // lat // per_tile):
            total = tail[t * per_tile]
            for i in range(1, per_tile):
                total = total + pltpu.roll(tail[t * per_tile + i], PIECE * i, axis=1)
            tail_ref[pl.ds(t * lat * SUB + r, lat, stride=SUB), :] = total

    def two(i, carry):
        prepare(2 * i + 1, odd_ref)
        cycle(2 * i, even_ref)
        prepare(2 * i + 2, even_ref)
        cycle(2 * i + 1, odd_ref)
        return carry

    @pl.when(pl.program_id(0) == 0)
    def _():
        prepare(0, even_ref)

    lax.fori_loop(0, SUB // 2, two, 0)

    halves = whole // LANES
    mains = 2 * WAVES_STEP * halves

    def deliver(owner, carry):
        quarter = 0
        for out_ref, quarters in zip(outs, groups):
            for q in range(quarters):
                for jj in range(2 * WAVES_STEP):
                    start = ((quarter * 2 * WAVES_STEP + jj) * lat + owner) * SUB
                    for h in range(halves):
                        piece = main_ref[h, pl.ds(pl.multiple_of(start, SUB), SUB), :]
                        out_ref[owner, 0, q, jj * halves + h] = piece.astype(jnp.bfloat16)
                for t in range(2):
                    start = ((quarter * 2 + t) * lat + owner) * SUB
                    value = tail_ref[pl.ds(pl.multiple_of(start, SUB), SUB), :]
                    out_ref[owner, 0, q, mains + t] = value.astype(jnp.bfloat16)
                quarter += 1
        return carry

    lax.fori_loop(0, lat, deliver, 0)


def forward(lat, first, blocks, groups, lengths, inverse, root, waves, sine, rows):
    cols, _, segment = rows.shape
    width = waves.shape[1]
    whole = cols // LANES * LANES
    tiles = 2 * WAVES_STEP * (whole // LANES) + 2
    smem = pl.BlockSpec(memory_space=pltpu.SMEM)
    small = pl.BlockSpec((1, width), lambda b: (0, 0))
    return pl.pallas_call(
        functools.partial(forward_kernel, lat, first, groups),
        grid=(blocks,),
        in_specs=[smem, smem, smem, small, small]
        + [pl.BlockSpec((cols, SUB, segment), lambda b: (0, b + first, 0))],
        out_specs=[
            pl.BlockSpec((lat, 1, q, tiles, SUB, LANES), lambda b: (0, b, 0, 0, 0, 0)) for q in groups
        ],
        out_shape=[
            jax.ShapeDtypeStruct((lat, blocks, q, tiles, SUB, LANES), jnp.bfloat16) for q in groups
        ],
        scratch_shapes=[
            pltpu.VMEM((segment // LANES, cols * SUB, LANES), jnp.float32),
            pltpu.VMEM((segment, width), jnp.bfloat16),
            pltpu.VMEM((segment, width), jnp.bfloat16),
            pltpu.VMEM((whole + LANES, width), jnp.float32),
            pltpu.VMEM((whole // LANES, width * SUB, LANES), jnp.float32),
            pltpu.VMEM((width // WAVES_STEP * SUB, LANES), jnp.float32),
        ],
        compiler_params=pltpu.CompilerParams(vmem_limit_bytes=58 * 2**20),
        cost_estimate=pl.CostEstimate(
            flops=2 * cols * segment * width * SUB * blocks,
            bytes_accessed=2 * cols * (segment + width) * SUB * blocks,
            transcendentals=0,
        ),
        name="forward_cycles",
    )(lengths, inverse, root, waves, sine, rows)


def middle_kernel(lat, parts, wave_ref, weight_ref, before_ref, legendre_ref, target_ref, *rest):
    ins = rest[: len(parts[0])]
    rest = rest[len(parts[0]) :]
    coeff_ref, loss_ref = rest[:2]
    outs, (grad_tail, flat_ref) = rest[2:-2], rest[-2:]
    cols, degrees = weight_ref.shape
    cycles = legendre_ref.shape[2]
    whole = cols // LANES * LANES
    halves = whole // LANES
    mains = 2 * WAVES_STEP * halves
    per_tile = WAVES_STEP
    rows = lat * SUB
    step = pl.program_id(0)
    degree = lax.broadcasted_iota(jnp.int32, (cols, degrees), 1)

    @pl.when(step == 0)
    def _():
        loss_ref[...] = before_ref[...]

    grad_tail[...] = jnp.zeros_like(grad_tail)
    flat_ref[cols // SUB * SUB :, :] = jnp.zeros(
        (flat_ref.shape[0] - cols // SUB * SUB, cycles), jnp.float32
    )

    def one(jj, carry):
        s, part = jj // 2, jj % 2
        tile, place = jj // per_tile, jj % per_tile
        pieces = []
        for ref, count in zip(ins, parts[0]):
            for b in range(count):
                lanes = [
                    ref[:, b, 0, jj * halves + h].reshape(rows, LANES) for h in range(halves)
                ]
                tail = ref[:, b, 0, mains + tile].reshape(rows, LANES).astype(jnp.float32)
                shift = lax.rem(LANES - PIECE * place, LANES)
                lanes.append(pltpu.roll(tail, shift, axis=1).astype(jnp.bfloat16))
                pieces.append(jnp.concatenate(lanes, axis=1))
        fourier = jnp.concatenate(pieces, axis=0)[:, :cols]
        basis = legendre_ref[s]
        coeffs = lax.dot_general(
            fourier, basis, (((0,), (1,)), ((), ())), preferred_element_type=jnp.float32
        )
        keep = degree >= wave_ref[step * WAVES_STEP + s]
        coeffs = jnp.where(keep, coeffs, 0.0)
        coeff_ref[s, part] = coeffs
        misfit = jnp.where(keep, coeffs - target_ref[s, part], 0.0)
        factor = jnp.where(wave_ref[step * WAVES_STEP + s] == 0, 1.0, 2.0)
        slope = (factor * weight_ref[...]) * misfit
        loss_ref[...] += jnp.sum(slope * misfit, axis=0, keepdims=True)
        grad = (2.0 * slope).astype(jnp.bfloat16)
        flat_ref[:cols, :] = jnp.dot(grad, basis, preferred_element_type=jnp.float32)
        main = flat_ref[:whole, :].T
        tail = flat_ref[whole:, :].T
        offset = 0
        for ref, count in zip(outs, parts[1]):
            for b in range(count):
                for h in range(halves):
                    value = main[offset : offset + rows, h * LANES : (h + 1) * LANES]
                    ref[:, b, 0, jj * halves + h] = value.astype(jnp.bfloat16).reshape(
                        lat, SUB, LANES
                    )
                offset += rows
        grad_tail[tile] += pltpu.roll(tail, PIECE * place, axis=1)
        return carry

    lax.fori_loop(0, 2 * WAVES_STEP, one, 0)
    lane = lax.broadcasted_iota(jnp.int32, (rows, LANES), 1)
    left = jnp.sum(loss_ref[...], axis=1, keepdims=True)
    total = jnp.zeros((rows, LANES), jnp.float32)
    for n in range(TERMS):
        term = left.astype(jnp.bfloat16).astype(jnp.float32)
        left = left - term
        total = jnp.where(lane == SPARE + n, term, total)
    for tile in range(2):
        offset = 0
        for ref, count in zip(outs, parts[1]):
            for b in range(count):
                value = grad_tail[tile, pl.ds(offset, rows), :]
                if tile == 0 and offset == 0:
                    value = value + total
                ref[:, b, 0, mains + tile] = value.astype(jnp.bfloat16).reshape(lat, SUB, LANES)
                offset += rows


def middle(lat, first, quarters, splits, waves, weight, before, legendre, target, arrays):
    cols, degrees = weight.shape
    cycles = legendre.shape[2]
    tiles = arrays[0][0].shape[3]
    whole = cols // LANES * LANES
    parts = (tuple(a.shape[1] for a, _ in arrays), tuple(splits))

    def tile_spec(count, start):
        return pl.BlockSpec(
            (lat, count, 1, tiles, SUB, LANES), lambda q: (0, 0, q + start, 0, 0, 0)
        )

    out_specs = [
        pl.BlockSpec((WAVES_STEP, 2, cols, degrees), lambda q: (q, 0, 0, 0)),
        pl.BlockSpec((1, degrees), lambda q: (0, 0)),
    ] + [tile_spec(count, 0) for count in splits]
    out_shape = [
        jax.ShapeDtypeStruct((quarters * WAVES_STEP, 2, cols, degrees), jnp.float32),
        jax.ShapeDtypeStruct((1, degrees), jnp.float32),
    ] + [
        jax.ShapeDtypeStruct((lat, count, quarters, tiles, SUB, LANES), jnp.bfloat16)
        for count in splits
    ]
    return pl.pallas_call(
        functools.partial(middle_kernel, lat, parts),
        grid=(quarters,),
        in_specs=[
            pl.BlockSpec(memory_space=pltpu.SMEM),
            pl.BlockSpec((cols, degrees), lambda q: (0, 0)),
            pl.BlockSpec((1, degrees), lambda q: (0, 0)),
            pl.BlockSpec((WAVES_STEP, degrees, cycles), lambda q: (q + first, 0, 0)),
            pl.BlockSpec((WAVES_STEP, 2, cols, degrees), lambda q: (q + first, 0, 0, 0)),
        ]
        + [tile_spec(a.shape[1], start) for a, start in arrays],
        out_specs=out_specs,
        out_shape=out_shape,
        scratch_shapes=[
            pltpu.VMEM((2, cycles, LANES), jnp.float32),
            pltpu.VMEM((whole + LANES, cycles), jnp.float32),
        ],
        compiler_params=pltpu.CompilerParams(vmem_limit_bytes=60 * 2**20),
        cost_estimate=pl.CostEstimate(
            flops=8 * cols * degrees * cycles * WAVES_STEP * quarters,
            bytes_accessed=20 * cols * degrees * WAVES_STEP * quarters,
            transcendentals=0,
        ),
        name="middle_waves",
    )(waves, weight, before, legendre, target, *[a for a, _ in arrays])


def backward_kernel(
    lat, first, groups, len_ref, inv_ref, root_ref, wave_ref, sine_ref, *rest
):
    ins = rest[: len(groups)]
    out_ref, rows_ref, even_ref, odd_ref, main_ref, tail_ref = rest[-6:]
    cols, _, segment = out_ref.shape
    width = even_ref.shape[1]
    whole = cols // LANES * LANES
    halves = whole // LANES
    mains = 2 * WAVES_STEP * halves
    per_tile = WAVES_STEP
    block = pl.program_id(0) + first

    def collect(owner, carry):
        quarter = 0
        for in_ref, quarters in zip(ins, groups):
            for q in range(quarters):
                for jj in range(2 * WAVES_STEP):
                    start = ((quarter * 2 * WAVES_STEP + jj) * lat + owner) * SUB
                    at = pl.ds(pl.multiple_of(start, SUB), SUB)
                    for h in range(halves):
                        value = in_ref[owner, 0, q, jj * halves + h].astype(jnp.float32)
                        main_ref[h, at, :] = value
                for t in range(2):
                    start = ((quarter * 2 + t) * lat + owner) * SUB
                    at = pl.ds(pl.multiple_of(start, SUB), SUB)
                    tail_ref[at, :] = in_ref[owner, 0, q, mains + t].astype(jnp.float32)
                quarter += 1
        return carry

    lax.fori_loop(0, lat, collect, 0)

    last = (first + pl.num_programs(0)) * SUB - 1

    def prepare(r, table_ref):
        slot = jnp.minimum(block * SUB + r, last)
        make_table(len_ref[slot], inv_ref[slot], root_ref[slot], wave_ref, sine_ref, table_ref)

    def cycle(r, table_ref):
        main = [main_ref[h, pl.ds(r, width, stride=SUB), :].T for h in range(halves)]
        pieces = []
        for t in range(width // lat // per_tile):
            value = tail_ref[pl.ds(t * lat * SUB + r, lat, stride=SUB), :]
            for i in range(per_tile):
                pieces.append(value if i == 0 else pltpu.roll(value, LANES - PIECE * i, axis=1))
        tail = jnp.concatenate(pieces, axis=0).T
        spectrum = jnp.concatenate([*main, tail[: cols - whole]], axis=0).astype(jnp.bfloat16)
        field = lax.dot_general(
            spectrum, table_ref[...], (((1,), (1,)), ((), ())), preferred_element_type=jnp.float32
        )
        length = len_ref[block * SUB + r]
        lane = lax.broadcasted_iota(jnp.int32, (cols, LANES), 1)
        for t in range(segment // LANES):
            piece = field[:, t * LANES : (t + 1) * LANES]
            piece = jnp.where(lane < length - t * LANES, piece, 0.0)
            rows_ref[t, pl.ds(r, cols, stride=SUB), :] = piece

    def two(i, carry):
        prepare(2 * i + 1, odd_ref)
        cycle(2 * i, even_ref)
        prepare(2 * i + 2, even_ref)
        cycle(2 * i + 1, odd_ref)
        return carry

    @pl.when(pl.program_id(0) == 0)
    def _():
        prepare(0, even_ref)

    lax.fori_loop(0, SUB // 2, two, 0)
    chunk = 12 if cols % 12 == 0 else 1

    def narrow(i, carry):
        start = pl.multiple_of(i * chunk * SUB, SUB)
        for t in range(segment // LANES):
            value = rows_ref[t, pl.ds(start, chunk * SUB), :].reshape(chunk, SUB, LANES)
            lanes = slice(t * LANES, (t + 1) * LANES)
            out_ref[pl.ds(i * chunk, chunk), :, lanes] = value.astype(jnp.bfloat16)
        return carry

    lax.fori_loop(0, cols // chunk, narrow, 0)


def backward(lat, first, blocks, lengths, inverse, root, waves, sine, arrays, shape, done):
    cols, _, segment = shape
    width = waves.shape[1]
    whole = cols // LANES * LANES
    tiles = arrays[0][0].shape[3]
    groups = tuple(a.shape[2] for a, _ in arrays)
    smem = pl.BlockSpec(memory_space=pltpu.SMEM)
    small = pl.BlockSpec((1, width), lambda b: (0, 0))

    def tile_spec(q, start):
        return pl.BlockSpec((lat, 1, q, tiles, SUB, LANES), lambda b: (0, b + start, 0, 0, 0, 0))

    extra = [] if done is None else [done]
    in_specs = [smem, smem, smem, small, small]
    in_specs += [tile_spec(a.shape[2], start) for a, start in arrays]
    in_specs += [pl.BlockSpec(memory_space=pl.ANY)] * len(extra)
    return pl.pallas_call(
        functools.partial(backward_kernel, lat, first, groups),
        grid=(blocks,),
        in_specs=in_specs,
        out_specs=pl.BlockSpec((cols, SUB, segment), lambda b: (0, b + first, 0)),
        out_shape=jax.ShapeDtypeStruct(shape, jnp.bfloat16),
        scratch_shapes=[
            pltpu.VMEM((segment // LANES, cols * SUB, LANES), jnp.float32),
            pltpu.VMEM((segment, width), jnp.bfloat16),
            pltpu.VMEM((segment, width), jnp.bfloat16),
            pltpu.VMEM((whole // LANES, width * SUB, LANES), jnp.float32),
            pltpu.VMEM((width // WAVES_STEP * SUB, LANES), jnp.float32),
        ],
        input_output_aliases={} if done is None else {5 + len(arrays): 0},
        compiler_params=pltpu.CompilerParams(vmem_limit_bytes=58 * 2**20),
        cost_estimate=pl.CostEstimate(
            flops=2 * cols * segment * width * SUB * blocks,
            bytes_accessed=2 * cols * (segment + width) * SUB * blocks,
            transcendentals=0,
        ),
        name="backward_cycles",
    )(lengths, inverse, root, waves, sine, *[a for a, _ in arrays], *extra)


def exchange(x):
    return lax.all_to_all(x, "lat", split_axis=0, concat_axis=0, tiled=True)


def per_device(lat, grid, cycle_ids, cycle_len, wave_ids, legendre, target, step_w, chan_w):
    _, batch_size, chan_count, cycle_dev, segment = grid.shape
    wave_count = wave_ids.shape[0]
    wave_dev, degrees, cycle_count = legendre.shape
    cols = batch_size * chan_count
    lat_index = lax.axis_index("lat")
    blocks = cycle_dev // SUB
    quarters = wave_dev // WAVES_STEP
    early = quarters // 2
    late = quarters - early
    rows = grid[0].reshape(cols, cycle_dev, segment)

    my_cycles = lax.dynamic_slice_in_dim(cycle_ids, lat_index * cycle_dev, cycle_dev)
    lengths = jnp.take(cycle_len, my_cycles)
    inverse = 1.0 / lengths.astype(jnp.float32)
    root = lax.rsqrt(lengths.astype(jnp.float32))
    by_slot = jnp.transpose(wave_ids.reshape(lat, wave_dev))
    waves = jnp.broadcast_to(by_slot[:, None, :], (wave_dev, 2, lat)).reshape(1, -1)
    sine = (jnp.arange(2 * wave_dev * lat, dtype=jnp.int32) // lat % 2).reshape(1, -1)
    tables = (lengths, inverse, root, waves, sine)

    (out0,) = forward(lat, 0, 1, (quarters,), *tables, rows)
    in0 = exchange(out0)
    out1, out2 = forward(lat, 1, blocks - 1, (early, late), *tables, rows)
    in1 = exchange(out1)
    in2 = exchange(out2)

    order = jnp.transpose(cycle_ids.reshape(lat, blocks, SUB), (1, 0, 2)).reshape(-1)
    pick = (jnp.arange(cycle_count, dtype=jnp.int32)[:, None] == order[None, :]).astype(jnp.bfloat16)
    basis = jnp.dot(
        legendre.reshape(wave_dev * degrees, cycle_count),
        pick,
        preferred_element_type=jnp.float32,
    )
    basis = basis.astype(jnp.bfloat16).reshape(wave_dev, degrees, cycle_count)
    my_waves = lax.dynamic_slice_in_dim(wave_ids, lat_index * wave_dev, wave_dev)
    weight = jnp.broadcast_to(step_w[0] * chan_w[None, :], (batch_size, chan_count))
    weight = jnp.broadcast_to(weight.reshape(cols, 1), (cols, degrees))
    goal = jnp.transpose(target[0].reshape(cols, 2, wave_dev, degrees), (2, 1, 0, 3))

    cut = early * WAVES_STEP
    nothing = jnp.zeros((1, degrees), jnp.float32)
    coeffs_a, loss_a, back0 = middle(
        lat, 0, early, (blocks,), my_waves[:cut], weight, nothing, basis, goal,
        [(in0, 0), (in1, 0)],
    )
    ret0 = exchange(back0)
    leave = ((blocks - 1) // 2, blocks - 1 - (blocks - 1) // 2, 1)
    coeffs_b, _, back1, back2, back3 = middle(
        lat, early, late, leave, my_waves[cut:], weight, loss_a, basis, goal,
        [(in0, early), (in2, 0)],
    )
    ret1 = exchange(back1)
    ret2 = exchange(back2)
    ret3 = exchange(back3)

    shape = (cols, cycle_dev, segment)
    field, start = None, 0
    for arrived, count in zip((ret1, ret2, ret3), leave):
        field = backward(lat, start, count, *tables, [(ret0, start), (arrived, 0)], shape, field)
        start += count
    field_grad = field.reshape(1, batch_size, chan_count, cycle_dev, segment)
    coeffs = jnp.concatenate([coeffs_a, coeffs_b], axis=0)
    coeff_out = jnp.transpose(coeffs, (2, 1, 0, 3)).reshape(
        1, batch_size, chan_count, 2, wave_dev, degrees
    )
    pieces = ret1[:, 0, late - 1, -2, 0, SPARE : SPARE + TERMS]
    loss_sum = jnp.sum(jnp.sum(pieces.astype(jnp.float32), axis=1))
    loss_sum = jnp.broadcast_to(loss_sum, (SUB, LANES))
    other = lax.ppermute(loss_sum, "fld", [(0, 1), (1, 0)])
    loss_sum = loss_sum[0, 0] + other[0, 0]
    term_count = STEPS * cols * wave_count * (wave_count + 1) // 2
    loss = loss_sum / jnp.float32(term_count)
    return (coeff_out, loss, field_grad)


def cycle_tables(lengths, waves, is_sine, segment):
    inner = math.gcd(segment, 32)
    outer = segment // inner
    length = lengths[:, None, None]
    wave = waves[None, None, :]
    coarse = (inner * jnp.arange(outer, dtype=jnp.int32))[None, :, None]
    fine = jnp.arange(inner, dtype=jnp.int32)[None, :, None]
    sin_a, cos_a = sin_cos(length, wave * coarse)
    sin_b, cos_b = sin_cos(length, wave * fine)
    scale = jnp.where(2 * wave < length, lax.rsqrt(length.astype(jnp.float32)), 0.0)
    sine = is_sine[None, None, :]
    first = jnp.where(sine, -sin_a, cos_a) * scale
    second = jnp.where(sine, -cos_a, -sin_a) * scale
    first, second, sin_b, cos_b = lax.optimization_barrier((first, second, sin_b, cos_b))
    table = first[:, :, None, :] * cos_b[:, None, :, :] + second[:, :, None, :] * sin_b[:, None, :, :]
    inside = (coarse[..., None] + fine[:, None]) < length[..., None]
    table = jnp.where(inside, table, 0.0).astype(jnp.bfloat16)
    return table.reshape(lengths.shape[0], segment, waves.shape[0])


def per_device_simple(lat, grid, cycle_ids, cycle_len, wave_ids, legendre, target, step_w, chan_w):
    _, batch_size, chan_count, cycle_dev, segment = grid.shape
    wave_count = wave_ids.shape[0]
    wave_dev, degrees, cycle_count = legendre.shape
    col_count = batch_size * chan_count
    lat_index = lax.axis_index("lat")
    my_cycles = lax.dynamic_slice_in_dim(cycle_ids, lat_index * cycle_dev, cycle_dev)
    lengths = jnp.take(cycle_len, my_cycles)

    pair = 2 * wave_dev
    by_owner = wave_ids.reshape(lat, 1, wave_dev)
    column_waves = jnp.broadcast_to(by_owner, (lat, 2, wave_dev)).reshape(-1)
    is_sine = (jnp.arange(lat * pair, dtype=jnp.int32) // wave_dev) % 2 == 1
    tables = cycle_tables(lengths, column_waves, is_sine, segment)
    tables = lax.optimization_barrier(tables)

    rows = grid[0].reshape(col_count, cycle_dev, segment)
    fourier = jnp.einsum("rkj,brk->rjb", tables, rows, preferred_element_type=jnp.float32)
    fourier = fourier.astype(jnp.bfloat16).reshape(cycle_dev, lat, pair, col_count)
    fourier = jnp.transpose(fourier, (1, 0, 2, 3))
    gathered = lax.all_to_all(fourier, "lat", split_axis=0, concat_axis=0, tiled=True)
    gathered = gathered.reshape(cycle_count, 2, wave_dev, col_count)

    legendre_cols = jnp.take(legendre, cycle_ids, axis=2)
    my_waves = lax.dynamic_slice_in_dim(wave_ids, lat_index * wave_dev, wave_dev)
    kept = jnp.arange(degrees, dtype=jnp.int32)[None, :] >= my_waves[:, None]
    kept = kept.astype(jnp.float32)[:, None, None, :]
    factor = jnp.where(my_waves == 0, 1.0, 2.0).astype(jnp.float32)
    weight_cols = jnp.broadcast_to(step_w[0] * chan_w[None, :], (batch_size, chan_count))
    weight = factor[:, None, None, None] * weight_cols.reshape(1, 1, col_count, 1)
    target_local = jnp.transpose(
        target[0].reshape(col_count, 2, wave_dev, degrees), (2, 1, 0, 3)
    )
    coeffs = jnp.einsum(
        "rpsb,snr->spbn", gathered, legendre_cols, preferred_element_type=jnp.float32
    )
    coeffs = coeffs * kept
    misfit = (coeffs - target_local) * kept
    partial_value = jnp.sum(weight * misfit * misfit)
    grad_coeff = (2.0 * weight * misfit).astype(jnp.bfloat16)
    back = jnp.einsum(
        "snr,spbn->sprb", legendre_cols, grad_coeff, preferred_element_type=jnp.float32
    )
    back = jnp.transpose(back.astype(jnp.bfloat16), (2, 1, 0, 3))
    back = back.reshape(lat, cycle_dev, pair, col_count)
    returned = lax.all_to_all(back, "lat", split_axis=0, concat_axis=0, tiled=True)
    returned = jnp.transpose(returned, (1, 0, 2, 3)).reshape(cycle_dev, lat * pair, col_count)
    field = jnp.einsum("rjb,rkj->brk", returned, tables, preferred_element_type=jnp.float32)
    field_grad = field.astype(jnp.bfloat16).reshape(
        1, batch_size, chan_count, cycle_dev, segment
    )
    coeff_out = jnp.transpose(coeffs, (2, 1, 0, 3)).reshape(
        1, batch_size, chan_count, 2, wave_dev, degrees
    )
    loss_sum = lax.psum(partial_value, ("lat", "fld"))
    term_count = STEPS * col_count * wave_count * (wave_count + 1) // 2
    loss = loss_sum / jnp.float32(term_count)
    return (coeff_out, loss, field_grad)


def tiled(lat, grid, legendre):
    _, batch_size, chan_count, cycle_dev, segment = grid.shape
    wave_dev, cols = legendre.shape[0], batch_size * chan_count
    spare = cols % LANES
    return (
        cycle_dev % SUB == 0
        and cycle_dev // SUB >= 3
        and wave_dev % (2 * WAVES_STEP) == 0
        and 2 * wave_dev * lat % LANES == 0
        and legendre.shape[2] % LANES == 0
        and lat % SUB == 0
        and segment % RUN == 0
        and segment % LANES == 0
        and cols > LANES
        and 0 < spare <= PIECE
        and PIECE * WAVES_STEP <= SPARE
        and lax.axis_size("fld") == 2
    )


def route(lat, grid, cycle_ids, cycle_len, wave_ids, legendre, *rest):
    run = per_device if tiled(lat, grid, legendre) else per_device_simple
    return run(lat, grid, cycle_ids, cycle_len, wave_ids, legendre, *rest)


def solution(mesh):
    lat = mesh.shape["lat"]
    return jax.shard_map(
        lambda *args: route(lat, *args),
        mesh=mesh,
        in_specs=(
            P("fld", None, None, "lat", None),
            P(),
            P(),
            P(),
            P("lat", None, None),
            P("fld", None, None, None, "lat", None),
            P("fld"),
            P(),
        ),
        out_specs=(P("fld", None, None, None, "lat", None), P(), P("fld", None, None, "lat", None)),
        check_vma=False,
    )
```
